32 devices in a mesh: seq: 16 (over z, x, core), grp: 2 (over y).
Axes of the slice: x: 2, y: 2, z: 4, core: 2. Of those that a mesh axis runs over, the one named last changes fastest.
Arguments:
- out_grad: bfloat16 [2, 3456, 1024], P('grp', 'seq'), may hold values from -6 to 6
- combine_logits: float32 [2, 3456, 64], P('grp', 'seq'), may hold values from -20 to 330
- expert_out: bfloat16 [2, 64, 1024], P('grp', 'seq'), may hold values from -6 to 6
- slot_in: bfloat16 [2, 64, 1024], P('grp', 'seq'), may hold values from -6 to 6
- router: bfloat16 [64, 1024], P('seq'), may hold values from -0.1875 to 0.1875
- w_gate: bfloat16 [64, 2048, 1024], P('seq', 'grp'), may hold values from -0.1875 to 0.1875
- w_up: bfloat16 [64, 2048, 1024], P('seq', 'grp'), may hold values from -0.1875 to 0.1875
- w_down: bfloat16 [64, 2048, 1024], P('seq', 'grp'), may hold values from -0.125 to 0.125
Outputs:
- token_grad: bfloat16 [2, 3456, 1024], P('grp', 'seq')
- slot_grad: float32 [2, 64, 1024], P('grp', 'seq')
- grad_gate: bfloat16 [64, 2048, 1024], P('seq', 'grp')
- grad_up: bfloat16 [64, 2048, 1024], P('seq', 'grp')
- grad_down: bfloat16 [64, 2048, 1024], P('seq', 'grp')
The draws below stay inside these ranges and needn't reach their ends.
All inputs are finite; a program needn't handle non-finite values.
Results may differ from the reference program's by a relative error of at most 0.028.
Values may be sent and summed in bfloat16 or wider, within the bound.
A program may use at most 128 MiB of HBM per device.

```python
import jax
import jax.numpy as jnp
from jax import lax

D = 1024
FF = 2048
EXPERTS = 64
TOKENS = 3456
SEQS = 2


def draw_combine_logits(key, part):
    keys = jax.random.split(key, 1)
    shape = (SEQS, TOKENS, EXPERTS)
    return jnp.clip(3.0 * jax.random.normal(keys[0], shape, jnp.float32), -18.0, 18.0)


def shard_levels(stream_key, shape, cuts, least, top_value):
    loudness = 1.0
    for dim, blocks in cuts:
        draws = jax.random.uniform(jax.random.fold_in(jax.random.fold_in(stream_key, 6), dim), (blocks,), jnp.float32, least / len(cuts), top_value / len(cuts))
        loudness = loudness * jnp.repeat(jnp.exp(draws), shape[dim] // blocks).reshape((-1,) + (1,) * (len(shape) - 1 - dim))
    return loudness


def centred(key, shape, spread, limit, cuts=(), kind=jnp.bfloat16):
    result = spread * jax.random.normal(key, shape, jnp.float32)
    if cuts:
        result = result * shard_levels(key, shape, cuts, -0.22, 0.18)
    return jnp.clip(result, -limit, limit).astype(kind)


def setup_inputs(seed: int = 0) -> dict:
    seeds = jax.random.split(jax.random.key(seed), 9)
    out_grad = centred(seeds[0], (SEQS, TOKENS, D), 1.0, 6.0, ((0, 2), (1, 16)))
    combine_logits = draw_combine_logits(jax.random.fold_in(seeds[8], 71), 0)
    expert_out = centred(seeds[2], (SEQS, EXPERTS, D), 1.0, 6.0, ((0, 2), (1, 16)))
    slot_in = centred(seeds[3], (SEQS, EXPERTS, D), 1.0, 6.0, ((0, 2), (1, 16)))
    router = centred(seeds[4], (EXPERTS, D), D ** -0.5, 0.1875, ((0, 16),))
    w_gate = centred(seeds[5], (EXPERTS, FF, D), D ** -0.5, 0.1875, ((0, 16), (1, 2)))
    w_up = centred(seeds[6], (EXPERTS, FF, D), D ** -0.5, 0.1875, ((0, 16), (1, 2)))
    w_down = centred(seeds[7], (EXPERTS, FF, D), FF ** -0.5, 0.125, ((0, 16), (1, 2)))
    return dict(out_grad=out_grad, combine_logits=combine_logits, expert_out=expert_out, slot_in=slot_in, router=router, w_gate=w_gate, w_up=w_up, w_down=w_down)


def sequence_part(items, router):
    grads, logits, outputs = items
    probs = jax.nn.softmax(logits, axis=-1)
    probs_bf = probs.astype(jnp.bfloat16)
    slot_out = lax.dot_general(probs_bf, grads, (((0,), (0,)), ((), ())), preferred_element_type=jnp.float32)
    weight_grad = lax.dot_general(grads, outputs, (((1,), (1,)), ((), ())), preferred_element_type=jnp.float32)
    centre = jnp.sum(weight_grad * probs, axis=-1, keepdims=True)
    logit_grad = (probs * (weight_grad - centre)).astype(jnp.bfloat16)
    token_grad = jnp.dot(logit_grad, router, preferred_element_type=jnp.float32).astype(jnp.bfloat16)
    return token_grad, slot_out.astype(jnp.bfloat16)


def expert_part(items):
    inputs, out_grads, w_gate, w_up, w_down = items
    dims = (((1,), (1,)), ((), ()))
    gate = lax.dot_general(inputs, w_gate, dims, preferred_element_type=jnp.float32)
    upper = lax.dot_general(inputs, w_up, dims, preferred_element_type=jnp.float32)
    sig = jax.nn.sigmoid(gate)
    hidden = (gate * sig * upper).astype(jnp.bfloat16)
    hidden_grad = lax.dot_general(out_grads, w_down, dims, preferred_element_type=jnp.float32)
    up_grad = (hidden_grad * gate * sig).astype(jnp.bfloat16)
    gate_grad = (hidden_grad * upper * sig * (1.0 + gate * (1.0 - sig))).astype(jnp.bfloat16)
    slot_grad = jnp.dot(gate_grad, w_gate, preferred_element_type=jnp.float32) + jnp.dot(up_grad, w_up, preferred_element_type=jnp.float32)
    outer = (((0,), (0,)), ((), ()))
    grad_gate = lax.dot_general(gate_grad, inputs, outer, preferred_element_type=jnp.float32).astype(jnp.bfloat16)
    grad_up = lax.dot_general(up_grad, inputs, outer, preferred_element_type=jnp.float32).astype(jnp.bfloat16)
    grad_down = lax.dot_general(hidden, out_grads, outer, preferred_element_type=jnp.float32).astype(jnp.bfloat16)
    return slot_grad, grad_gate, grad_up, grad_down


def reference(out_grad, combine_logits, expert_out, slot_in, router, w_gate, w_up, w_down):
    token_grad, slot_out_bf = lax.map(lambda items: sequence_part(items, router), (out_grad, combine_logits, expert_out))
    per_expert = (jnp.transpose(slot_in, (1, 0, 2)), jnp.transpose(slot_out_bf, (1, 0, 2)), w_gate, w_up, w_down)
    slot_grad, grad_gate, grad_up, grad_down = lax.map(expert_part, per_expert)
    return token_grad, jnp.transpose(slot_grad, (1, 0, 2)), grad_gate, grad_up, grad_down
```

```python
import functools

import jax
import jax.numpy as jnp
from jax import lax
from jax.experimental import pallas as pl
from jax.experimental.pallas import tpu as pltpu
from jax.sharding import PartitionSpec as P

MESH = pl.DeviceIdType.MESH
F32 = jnp.float32
BF16 = jnp.bfloat16
NT = (((1,), (1,)), ((), ()))
TN = (((0,), (0,)), ((), ()))


def rows_of(ref, count):
    return jnp.concatenate([ref[i].astype(F32) for i in range(count)], axis=0).astype(BF16)


def exchange_kernel(
    nseq, ngrp,
    grad_hbm, logit_hbm, eout_hbm, slot_hbm, router_hbm, gate_hbm, up_hbm, down_hbm,
    gate_w, up_w, down_w, grad, probs_ref, acts_ref, hid_ref, pair_ref, eout_ref, rout_ref,
    part_out, part_in, pieces, slots, outs,
    load_sem, w_sem, part_ssem, part_rsem, piece_ssem, piece_rsem,
    slot_ssem, slot_rsem, out_ssem, out_rsem,
):
    s_me = lax.axis_index("seq")
    g_me = lax.axis_index("grp")
    experts = slots.shape[1]

    barrier = pltpu.get_barrier_semaphore()

    def greet_seq(d, c):
        pl.semaphore_signal(barrier, inc=1, device_id={"seq": lax.rem(s_me + d, nseq)}, device_id_type=MESH)
        return c

    def greet_grp(d, c):
        pl.semaphore_signal(barrier, inc=1, device_id={"grp": lax.rem(g_me + d, ngrp)}, device_id_type=MESH)
        return c

    lax.fori_loop(1, ngrp, greet_grp, 0)
    lax.fori_loop(1, nseq, greet_seq, 0)

    loads = [
        pltpu.make_async_copy(logit_hbm, probs_ref, load_sem.at[0]),
        pltpu.make_async_copy(grad_hbm.at[0], grad, load_sem.at[1]),
        pltpu.make_async_copy(slot_hbm.at[0], slots.at[g_me], load_sem.at[2]),
        pltpu.make_async_copy(eout_hbm.at[0], pieces.at[s_me, 0], load_sem.at[3]),
        pltpu.make_async_copy(router_hbm, pieces.at[s_me, 1], load_sem.at[4]),
    ]
    for c in loads:
        c.start()
    w_loads = {}
    for m, (src, dst) in enumerate(((gate_hbm, gate_w), (up_hbm, up_w), (down_hbm, down_w))):
        for e in range(experts):
            w_loads[m, e] = pltpu.make_async_copy(src.at[e], dst.at[e], w_sem.at[m, e])

    def part_copy(d):
        to = lax.rem(s_me + d, nseq)
        return pltpu.make_async_remote_copy(
            src_ref=part_out.at[to], dst_ref=part_in.at[s_me],
            send_sem=part_ssem.at[to], recv_sem=part_rsem.at[s_me],
            device_id={"seq": to}, device_id_type=MESH)

    def piece_copy(d):
        to = lax.rem(s_me + d, nseq)
        return pltpu.make_async_remote_copy(
            src_ref=pieces.at[s_me], dst_ref=pieces.at[s_me],
            send_sem=piece_ssem.at[to], recv_sem=piece_rsem.at[s_me],
            device_id={"seq": to}, device_id_type=MESH)

    def grp_copy(d, buf, ssem, rsem):
        to = lax.rem(g_me + d, ngrp)
        return pltpu.make_async_remote_copy(
            src_ref=buf.at[g_me], dst_ref=buf.at[g_me],
            send_sem=ssem.at[to], recv_sem=rsem.at[g_me],
            device_id={"grp": to}, device_id_type=MESH)

    def seq_arrived(d, buf, rsem, ssem):
        at = lax.rem(s_me + d, nseq)
        pltpu.make_async_remote_copy(
            src_ref=buf.at[at], dst_ref=buf.at[at], send_sem=ssem.at[at], recv_sem=rsem.at[at],
            device_id={"seq": at}, device_id_type=MESH).wait_recv()

    def grp_arrived(d, buf, rsem, ssem):
        at = lax.rem(g_me + d, ngrp)
        pltpu.make_async_remote_copy(
            src_ref=buf.at[at], dst_ref=buf.at[at], send_sem=ssem.at[at], recv_sem=rsem.at[at],
            device_id={"grp": at}, device_id_type=MESH).wait_recv()

    def each(low, high, fn):
        def step(d, c):
            fn(d)
            return c
        lax.fori_loop(low, high, step, 0)

    loads[0].wait()
    z = probs_ref[...]
    z = jnp.exp(z - jnp.max(z, axis=0, keepdims=True))
    probs = z / jnp.sum(z, axis=0, keepdims=True)
    probs_ref[...] = probs
    loads[1].wait()
    for e in range(experts):
        w_loads[0, e].start()
        w_loads[1, e].start()
    for e in range(experts):
        w_loads[2, e].start()
    share = jnp.dot(probs.astype(BF16), grad[...], preferred_element_type=F32)
    for j in range(nseq):
        part_out[j] = share[j * experts:(j + 1) * experts].astype(BF16)
    part_in[s_me] = part_out[s_me]
    for c in loads[2:]:
        c.wait()

    pl.semaphore_wait(barrier, (nseq - 1) + (ngrp - 1))
    each(1, ngrp, lambda d: grp_copy(d, slots, slot_ssem, slot_rsem).start())
    each(1, nseq, lambda d: part_copy(d).start())
    each(1, nseq, lambda d: piece_copy(d).start())

    rows = ngrp * experts
    width = gate_w.shape[1]
    own = lax.rem(lax.broadcasted_iota(jnp.int32, (rows, width), 0), experts)

    each(1, ngrp, lambda d: grp_arrived(d, slots, slot_rsem, slot_ssem))
    x = rows_of(slots, ngrp)
    pair_ref[0] = x

    gate = jnp.zeros((rows, width), F32)
    upper = jnp.zeros((rows, width), F32)

    def project(e, gate, upper):
        w_loads[0, e].wait()
        gate = jnp.where(own == e, lax.dot_general(x, gate_w[e], NT, preferred_element_type=F32), gate)
        w_loads[1, e].wait()
        upper = jnp.where(own == e, lax.dot_general(x, up_w[e], NT, preferred_element_type=F32), upper)
        return gate, upper

    early = experts // 2
    for e in range(early):
        gate, upper = project(e, gate, upper)

    each(1, nseq, lambda d: seq_arrived(d, part_in, part_rsem, part_ssem))
    outs[g_me] = jnp.sum(part_in[...].astype(F32), axis=0).astype(BF16)
    each(1, ngrp, lambda d: grp_copy(d, outs, out_ssem, out_rsem).start())

    for e in range(early, experts):
        gate, upper = project(e, gate, upper)
    sig = jax.nn.sigmoid(gate)
    act = gate * sig
    hid_ref[...] = (act * upper).astype(BF16)
    acts_ref[0] = upper * sig * (1.0 + gate * (1.0 - sig))
    acts_ref[1] = act

    for e in range(experts):
        w_loads[2, e].wait()
    each(1, ngrp, lambda d: grp_arrived(d, outs, out_rsem, out_ssem))
    pair_ref[1] = rows_of(outs, ngrp)

    each(1, nseq, lambda d: seq_arrived(d, pieces, piece_rsem, piece_ssem))
    eout_ref[...] = rows_of(pieces.at[:, 0], nseq)
    rout_ref[...] = rows_of(pieces.at[:, 1], nseq)

    each(1, nseq, lambda d: part_copy(d).wait_send())
    each(1, nseq, lambda d: piece_copy(d).wait_send())
    each(1, ngrp, lambda d: grp_copy(d, slots, slot_ssem, slot_rsem).wait_send())
    each(1, ngrp, lambda d: grp_copy(d, outs, out_ssem, out_rsem).wait_send())


def mxu_outer(a, v, cut, store):
    for j in range(a.shape[1] // cut):
        at = slice(j * cut, (j + 1) * cut)
        store(j, lax.dot_general(a[:, at], v, TN, preferred_element_type=F32).astype(BF16))


def vpu_outer(a_cols, v_rows, cut, store):
    for j in range(a_cols[0].shape[0] // cut):
        at = slice(j * cut, (j + 1) * cut)
        total = a_cols[0][at] * v_rows[0]
        for a, v in zip(a_cols[1:], v_rows[1:]):
            total += a[at] * v
        store(j, total.astype(BF16))


def first_kernel(
    experts, cut,
    gate_w, up_w, down_w, acts_ref, hid_ref, pair_ref,
    gg_ref, mine_ref, send_ref, gu_hbm, gd_hbm,
    staged, sem,
):
    outs = (gd_hbm, gu_hbm)
    rows, width = hid_ref.shape
    ngrp = rows // experts
    own = lax.rem(lax.broadcasted_iota(jnp.int32, (rows, width), 0), experts)

    def chunk(k, e, j):
        at = pl.ds(j * cut, cut)
        return pltpu.make_async_copy(staged.at[k, e, at], outs[k].at[e, at], sem.at[k, e, j])

    def put(k, e):
        def store(j, value):
            staged[k, e, j * cut:(j + 1) * cut] = value
            chunk(k, e, j).start()
        return store

    x, so = pair_ref[0], pair_ref[1]
    hid = hid_ref[...].astype(F32)
    total = jnp.zeros((rows, x.shape[1]), F32)
    gate_all = jnp.zeros((rows, width), F32)
    for e in range(experts):
        mine = own == e
        mxu_outer(jnp.where(mine, hid, 0.0).astype(BF16), so, cut, put(0, e))
        hgrad = lax.dot_general(so, down_w[e], NT, preferred_element_type=F32)
        up_grad = jnp.where(mine, hgrad * acts_ref[1], 0.0).astype(BF16)
        gate_f = jnp.where(mine, hgrad * acts_ref[0], 0.0)
        gate_all += gate_f
        mxu_outer(up_grad, x, cut, put(1, e))
        total += jnp.dot(gate_f.astype(BF16), gate_w[e], preferred_element_type=F32)
        total += jnp.dot(up_grad, up_w[e], preferred_element_type=F32)
    gg_ref[...] = gate_all.astype(BF16)
    g_me = lax.axis_index("grp")
    for d in range(ngrp):
        at = lax.rem(g_me + d, ngrp)
        piece = jnp.zeros((experts, total.shape[1]), F32)
        for g in range(ngrp):
            piece = jnp.where(at == g, total[g * experts:(g + 1) * experts], piece)
        if d == 0:
            mine_ref[...] = piece
        else:
            send_ref[d - 1] = piece.astype(BF16)
    for k in range(2):
        for e in range(experts):
            for j in range(width // cut):
                chunk(k, e, j).wait()


def second_kernel(
    experts, cut,
    gg_ref, pair_ref, probs_ref, grad_ref, eout_ref, rout_ref,
    tgrad_hbm, gg_hbm,
    staged, tokens, sem, small_sem,
):
    rows, width = gg_ref.shape
    own = lax.rem(lax.broadcasted_iota(jnp.int32, (rows, width), 0), experts)

    def chunk(e, j):
        at = pl.ds(j * cut, cut)
        return pltpu.make_async_copy(staged.at[e, at], gg_hbm.at[e, at], sem.at[e, j])

    def put(e):
        def store(j, value):
            staged[e, j * cut:(j + 1) * cut] = value
            chunk(e, j).start()
        return store

    x = pair_ref[0]
    gate_grad = gg_ref[...].astype(F32)
    for e in range(experts):
        mxu_outer(jnp.where(own == e, gate_grad, 0.0).astype(BF16), x, cut, put(e))
        if e == 0:
            wgrad = lax.dot_general(eout_ref[...], grad_ref[...], NT, preferred_element_type=F32)
            p = probs_ref[...]
            centre = jnp.sum(wgrad * p, axis=0, keepdims=True)
            lgrad = (p * (wgrad - centre)).astype(BF16)
            tokens[...] = lax.dot_general(lgrad, rout_ref[...], TN, preferred_element_type=F32).astype(BF16)
            small = pltpu.make_async_copy(tokens, tgrad_hbm.at[0], small_sem.at[0])
            small.start()
    for e in range(experts):
        for j in range(width // cut):
            chunk(e, j).wait()
    small.wait()


def per_device(nseq, ngrp, out_grad, combine_logits, expert_out, slot_in, router, w_gate, w_up, w_down):
    _, tokens, dim = out_grad.shape
    total_experts = combine_logits.shape[2]
    experts, width, _ = w_gate.shape
    rows = ngrp * experts
    DMA = pltpu.SemaphoreType.DMA
    hspec = pl.BlockSpec(memory_space=pltpu.HBM)
    vspec = pl.BlockSpec(memory_space=pltpu.VMEM)
    weights = jax.ShapeDtypeStruct((experts, width, dim), BF16)
    gate_w, up_w, down_w, grad, probs, acts, hid, pair, eout, rout = pl.pallas_call(
        functools.partial(exchange_kernel, nseq, ngrp),
        out_shape=(
            weights, weights, weights,
            jax.ShapeDtypeStruct((tokens, dim), BF16),
            jax.ShapeDtypeStruct((total_experts, tokens), F32),
            jax.ShapeDtypeStruct((2, rows, width), F32),
            jax.ShapeDtypeStruct((rows, width), BF16),
            jax.ShapeDtypeStruct((2, rows, dim), BF16),
            jax.ShapeDtypeStruct((total_experts, dim), BF16),
            jax.ShapeDtypeStruct((total_experts, dim), BF16),
        ),
        in_specs=[hspec] * 8,
        out_specs=(vspec,) * 10,
        scratch_shapes=[
            pltpu.VMEM((nseq, experts, dim), BF16),
            pltpu.VMEM((nseq, experts, dim), BF16),
            pltpu.VMEM((nseq, 2, experts, dim), BF16),
            pltpu.VMEM((ngrp, experts, dim), BF16),
            pltpu.VMEM((ngrp, experts, dim), BF16),
            DMA((5,)), DMA((3, experts)),
            DMA((nseq,)), DMA((nseq,)), DMA((nseq,)), DMA((nseq,)),
            DMA((ngrp,)), DMA((ngrp,)), DMA((ngrp,)), DMA((ngrp,)),
        ],
        compiler_params=pltpu.CompilerParams(
            collective_id=0, has_side_effects=True, vmem_limit_bytes=8 * 1024 * 1024),
        name="exchange",
    )(*(pltpu.with_memory_space_constraint(a, pltpu.HBM) for a in (
        out_grad, jnp.transpose(combine_logits[0]), expert_out, slot_in, router, w_gate, w_up, w_down)))

    cut = 256 if width % 256 == 0 else width
    gate_grad, mine, sends, grad_up, grad_down = pl.pallas_call(
        functools.partial(first_kernel, experts, cut),
        out_shape=(
            jax.ShapeDtypeStruct((rows, width), BF16),
            jax.ShapeDtypeStruct((experts, dim), F32),
            jax.ShapeDtypeStruct((max(ngrp - 1, 1), experts, dim), BF16),
            weights, weights,
        ),
        in_specs=[vspec] * 6,
        out_specs=(vspec,) * 3 + (hspec,) * 2,
        scratch_shapes=[
            pltpu.VMEM((2, experts, width, dim), BF16),
            DMA((2, experts, width // cut)),
        ],
        compiler_params=pltpu.CompilerParams(vmem_limit_bytes=20 * 1024 * 1024),
        name="first",
    )(gate_w, up_w, down_w, acts, hid, pair)

    got = [
        lax.ppermute(sends[d - 1], "grp", [(g, (g + d) % ngrp) for g in range(ngrp)])
        for d in range(1, ngrp)
    ]

    token_grad, grad_gate = pl.pallas_call(
        functools.partial(second_kernel, experts, cut),
        out_shape=(jax.ShapeDtypeStruct((1, tokens, dim), BF16), weights),
        in_specs=[vspec] * 6,
        out_specs=(hspec,) * 2,
        scratch_shapes=[
            pltpu.VMEM((experts, width, dim), BF16),
            pltpu.VMEM((tokens, dim), BF16),
            DMA((experts, width // cut)),
            DMA((1,)),
        ],
        compiler_params=pltpu.CompilerParams(vmem_limit_bytes=12 * 1024 * 1024),
        cost_estimate=pl.CostEstimate(
            flops=0, bytes_accessed=experts * width * dim * 2, transcendentals=0),
        name="second",
    )(gate_grad, pair, probs, grad, eout, rout)
    slot_grad = mine
    for part in got:
        slot_grad = slot_grad + part.astype(F32)
    return token_grad, slot_grad[None], grad_gate, grad_up, grad_down


def solution(mesh):
    return jax.shard_map(
        functools.partial(per_device, mesh.shape["seq"], mesh.shape["grp"]),
        mesh=mesh,
        in_specs=(
            P("grp", "seq", None),
            P("grp", "seq", None),
            P("grp", "seq", None),
            P("grp", "seq", None),
            P("seq", None),
            P("seq", "grp", None),
            P("seq", "grp", None),
            P("seq", "grp", None),
        ),
        out_specs=(
            P("grp", "seq", None),
            P("grp", "seq", None),
            P("seq", "grp", None),
            P("seq", "grp", None),
            P("seq", "grp", None),
        ),
        check_vma=False,
    )
```

```python
import functools

import jax
import jax.numpy as jnp
from jax import lax
from jax.experimental import pallas as pl
from jax.experimental.pallas import tpu as pltpu
from jax.sharding import PartitionSpec as P

MESH = pl.DeviceIdType.MESH
F32 = jnp.float32
BF16 = jnp.bfloat16
NT = (((1,), (1,)), ((), ()))
TN = (((0,), (0,)), ((), ()))


def rows_of(ref, count):
    return jnp.concatenate([ref[i].astype(F32) for i in range(count)], axis=0).astype(BF16)


def exchange_kernel(
    nseq, ngrp,
    grad_hbm, logit_hbm, eout_hbm, slot_hbm, router_hbm, gate_hbm, up_hbm, down_hbm,
    gate_w, up_w, down_w, grad, probs_ref, acts_ref, hid_ref, pair_ref, eout_ref, rout_ref,
    part_out, part_in, pieces, slots, outs,
    load_sem, w_sem, part_ssem, part_rsem, piece_ssem, piece_rsem,
    slot_ssem, slot_rsem, out_ssem, out_rsem,
):
    s_me = lax.axis_index("seq")
    g_me = lax.axis_index("grp")
    experts = slots.shape[1]

    barrier = pltpu.get_barrier_semaphore()

    def greet_seq(d, c):
        pl.semaphore_signal(barrier, inc=1, device_id={"seq": lax.rem(s_me + d, nseq)}, device_id_type=MESH)
        return c

    def greet_grp(d, c):
        pl.semaphore_signal(barrier, inc=1, device_id={"grp": lax.rem(g_me + d, ngrp)}, device_id_type=MESH)
        return c

    lax.fori_loop(1, ngrp, greet_grp, 0)
    lax.fori_loop(1, nseq, greet_seq, 0)

    loads = [
        pltpu.make_async_copy(logit_hbm, probs_ref, load_sem.at[0]),
        pltpu.make_async_copy(grad_hbm.at[0], grad, load_sem.at[1]),
        pltpu.make_async_copy(slot_hbm.at[0], slots.at[g_me], load_sem.at[2]),
        pltpu.make_async_copy(eout_hbm.at[0], pieces.at[s_me, 0], load_sem.at[3]),
        pltpu.make_async_copy(router_hbm, pieces.at[s_me, 1], load_sem.at[4]),
    ]
    for c in loads:
        c.start()
    w_loads = {}
    for m, (src, dst) in enumerate(((gate_hbm, gate_w), (up_hbm, up_w), (down_hbm, down_w))):
        for e in range(experts):
            w_loads[m, e] = pltpu.make_async_copy(src.at[e], dst.at[e], w_sem.at[m, e])

    def part_copy(d):
        to = lax.rem(s_me + d, nseq)
        return pltpu.make_async_remote_copy(
            src_ref=part_out.at[to], dst_ref=part_in.at[s_me],
            send_sem=part_ssem.at[to], recv_sem=part_rsem.at[s_me],
            device_id={"seq": to}, device_id_type=MESH)

    def piece_copy(d):
        to = lax.rem(s_me + d, nseq)
        return pltpu.make_async_remote_copy(
            src_ref=pieces.at[s_me], dst_ref=pieces.at[s_me],
            send_sem=piece_ssem.at[to], recv_sem=piece_rsem.at[s_me],
            device_id={"seq": to}, device_id_type=MESH)

    def grp_copy(d, buf, ssem, rsem):
        to = lax.rem(g_me + d, ngrp)
        return pltpu.make_async_remote_copy(
            src_ref=buf.at[g_me], dst_ref=buf.at[g_me],
            send_sem=ssem.at[to], recv_sem=rsem.at[g_me],
            device_id={"grp": to}, device_id_type=MESH)

    def seq_arrived(d, buf, rsem, ssem):
        at = lax.rem(s_me + d, nseq)
        pltpu.make_async_remote_copy(
            src_ref=buf.at[at], dst_ref=buf.at[at], send_sem=ssem.at[at], recv_sem=rsem.at[at],
            device_id={"seq": at}, device_id_type=MESH).wait_recv()

    def grp_arrived(d, buf, rsem, ssem):
        at = lax.rem(g_me + d, ngrp)
        pltpu.make_async_remote_copy(
            src_ref=buf.at[at], dst_ref=buf.at[at], send_sem=ssem.at[at], recv_sem=rsem.at[at],
            device_id={"grp": at}, device_id_type=MESH).wait_recv()

    def each(low, high, fn):
        def step(d, c):
            fn(d)
            return c
        lax.fori_loop(low, high, step, 0)

    loads[0].wait()
    z = probs_ref[...]
    z = jnp.exp(z - jnp.max(z, axis=0, keepdims=True))
    probs = z / jnp.sum(z, axis=0, keepdims=True)
    probs_ref[...] = probs
    loads[1].wait()
    for e in range(experts):
        w_loads[0, e].start()
        w_loads[1, e].start()
    for e in range(experts):
        w_loads[2, e].start()
    share = jnp.dot(probs.astype(BF16), grad[...], preferred_element_type=F32)
    for j in range(nseq):
        part_out[j] = share[j * experts:(j + 1) * experts].astype(BF16)
    part_in[s_me] = part_out[s_me]
    for c in loads[2:]:
        c.wait()

    pl.semaphore_wait(barrier, (nseq - 1) + (ngrp - 1))
    each(1, ngrp, lambda d: grp_copy(d, slots, slot_ssem, slot_rsem).start())
    each(1, nseq, lambda d: part_copy(d).start())
    each(1, nseq, lambda d: piece_copy(d).start())

    rows = ngrp * experts
    width = gate_w.shape[1]
    own = lax.rem(lax.broadcasted_iota(jnp.int32, (rows, width), 0), experts)

    each(1, ngrp, lambda d: grp_arrived(d, slots, slot_rsem, slot_ssem))
    x = rows_of(slots, ngrp)
    pair_ref[0] = x

    gate = jnp.zeros((rows, width), F32)
    upper = jnp.zeros((rows, width), F32)

    def project(e, gate, upper):
        w_loads[0, e].wait()
        gate = jnp.where(own == e, lax.dot_general(x, gate_w[e], NT, preferred_element_type=F32), gate)
        w_loads[1, e].wait()
        upper = jnp.where(own == e, lax.dot_general(x, up_w[e], NT, preferred_element_type=F32), upper)
        return gate, upper

    early = experts // 2
    for e in range(early):
        gate, upper = project(e, gate, upper)

    each(1, nseq, lambda d: seq_arrived(d, part_in, part_rsem, part_ssem))
    outs[g_me] = jnp.sum(part_in[...].astype(F32), axis=0).astype(BF16)
    each(1, ngrp, lambda d: grp_copy(d, outs, out_ssem, out_rsem).start())

    for e in range(early, experts):
        gate, upper = project(e, gate, upper)
    sig = jax.nn.sigmoid(gate)
    act = gate * sig
    hid_ref[...] = (act * upper).astype(BF16)
    acts_ref[0] = upper * sig * (1.0 + gate * (1.0 - sig))
    acts_ref[1] = act

    for e in range(experts):
        w_loads[2, e].wait()
    each(1, ngrp, lambda d: grp_arrived(d, outs, out_rsem, out_ssem))
    pair_ref[1] = rows_of(outs, ngrp)

    each(1, nseq, lambda d: seq_arrived(d, pieces, piece_rsem, piece_ssem))
    eout_ref[...] = rows_of(pieces.at[:, 0], nseq)
    rout_ref[...] = rows_of(pieces.at[:, 1], nseq)

    each(1, nseq, lambda d: part_copy(d).wait_send())
    each(1, nseq, lambda d: piece_copy(d).wait_send())
    each(1, ngrp, lambda d: grp_copy(d, slots, slot_ssem, slot_rsem).wait_send())
    each(1, ngrp, lambda d: grp_copy(d, outs, out_ssem, out_rsem).wait_send())


def mxu_outer(a, v, dst):
    dst[...] = lax.dot_general(a, v, TN, preferred_element_type=F32).astype(BF16)


def picker(experts, e, rows, lanes=128):
    row = lax.broadcasted_iota(jnp.int32, (rows, lanes * (rows // experts)), 0)
    lane = lax.broadcasted_iota(jnp.int32, (rows, lanes * (rows // experts)), 1)
    return jnp.where(row == (lane // lanes) * experts + e, 1.0, 0.0).astype(BF16)


def vpu_outer(experts, e, a, v, dst, lanes=128, step=16):
    rows, dim = v.shape
    spread = lax.dot_general(a, picker(experts, e, rows, lanes), TN, preferred_element_type=F32).astype(BF16)
    tiles = [
        [jnp.broadcast_to(v[r:r + 1, l:l + lanes], (step, lanes)) for l in range(0, dim, lanes)]
        for r in range(e, rows, experts)
    ]
    for i in range(0, a.shape[1], step):
        out = []
        for l in range(dim // lanes):
            total = None
            for g, row in enumerate(tiles):
                term = spread[i:i + step, g * lanes:(g + 1) * lanes] * row[l]
                total = term if total is None else total + term
            out.append(total)
        dst[i:i + step] = jnp.concatenate(out, axis=1)


def first_kernel(
    experts, cut,
    gate_w, up_w, down_w, acts_ref, hid_ref, pair_ref,
    gg_ref, mine_ref, send_ref, gu_hbm, gd_hbm,
    staged, sem,
):
    outs = (gd_hbm, gu_hbm)
    rows, width = hid_ref.shape
    ngrp = rows // experts
    own = lax.rem(lax.broadcasted_iota(jnp.int32, (rows, cut), 0), experts)
    x, so = pair_ref[0], pair_ref[1]

    def chunk(k, e, j):
        at = pl.ds(j * cut, cut)
        return pltpu.make_async_copy(staged.at[k, e, at], outs[k].at[e, at], sem.at[k, e, j])

    def put(k, e, j, a, v):
        vpu_outer(experts, e, a, v, staged.at[k, e, pl.ds(j * cut, cut)])
        chunk(k, e, j).start()

    def spread(e, j, gate_grad, up_grad, total):
        at = slice(j * cut, (j + 1) * cut)
        total += jnp.dot(gate_grad, gate_w[e, at], preferred_element_type=F32)
        total += jnp.dot(up_grad, up_w[e, at], preferred_element_type=F32)
        put(1, e, j, up_grad, x)
        return total

    total = jnp.zeros((rows, x.shape[1]), F32)
    gate_all = [jnp.zeros((rows, cut), F32)] * (width // cut)
    late = []
    for e in range(experts):
        for j in range(width // cut):
            at = slice(j * cut, (j + 1) * cut)
            hgrad = lax.dot_general(so, down_w[e, at], NT, preferred_element_type=F32)
            put(0, e, j, hid_ref[:, at], so)
            gate_f = jnp.where(own == e, hgrad * acts_ref[0, :, at], 0.0)
            gate_all[j] += gate_f
            up_grad = jnp.where(own == e, hgrad * acts_ref[1, :, at], 0.0).astype(BF16)
            late.append((e, j, gate_f.astype(BF16), up_grad))
            if len(late) > 1:
                total = spread(*late.pop(0), total)
    for item in late:
        total = spread(*item, total)
    for j in range(width // cut):
        gg_ref[:, j * cut:(j + 1) * cut] = gate_all[j].astype(BF16)
    g_me = lax.axis_index("grp")
    for d in range(ngrp):
        at = lax.rem(g_me + d, ngrp)
        piece = jnp.zeros((experts, total.shape[1]), F32)
        for g in range(ngrp):
            piece = jnp.where(at == g, total[g * experts:(g + 1) * experts], piece)
        if d == 0:
            mine_ref[...] = piece
        else:
            send_ref[d - 1] = piece.astype(BF16)
    for k in range(2):
        for e in range(experts):
            for j in range(width // cut):
                chunk(k, e, j).wait()


def second_kernel(
    experts, cut,
    gg_ref, pair_ref, probs_ref, grad_ref, eout_ref, rout_ref,
    tgrad_hbm, gg_hbm,
    staged, tokens, sem, small_sem,
):
    rows, width = gg_ref.shape

    def chunk(e, j):
        at = pl.ds(j * cut, cut)
        return pltpu.make_async_copy(staged.at[e, at], gg_hbm.at[e, at], sem.at[e, j])

    x = pair_ref[0]
    small = None
    for e in range(experts):
        for j in range(width // cut):
            at = slice(j * cut, (j + 1) * cut)
            vpu_outer(experts, e, gg_ref[:, at], x, staged.at[e, at])
            chunk(e, j).start()
            if small is None:
                wgrad = lax.dot_general(eout_ref[...], grad_ref[...], NT, preferred_element_type=F32)
                p = probs_ref[...]
                centre = jnp.sum(wgrad * p, axis=0, keepdims=True)
                lgrad = (p * (wgrad - centre)).astype(BF16)
                tokens[...] = lax.dot_general(lgrad, rout_ref[...], TN, preferred_element_type=F32).astype(BF16)
                small = pltpu.make_async_copy(tokens, tgrad_hbm.at[0], small_sem.at[0])
                small.start()
    for e in range(experts):
        for j in range(width // cut):
            chunk(e, j).wait()
    small.wait()


def per_device(nseq, ngrp, out_grad, combine_logits, expert_out, slot_in, router, w_gate, w_up, w_down):
    _, tokens, dim = out_grad.shape
    total_experts = combine_logits.shape[2]
    experts, width, _ = w_gate.shape
    rows = ngrp * experts
    DMA = pltpu.SemaphoreType.DMA
    hspec = pl.BlockSpec(memory_space=pltpu.HBM)
    vspec = pl.BlockSpec(memory_space=pltpu.VMEM)
    weights = jax.ShapeDtypeStruct((experts, width, dim), BF16)
    gate_w, up_w, down_w, grad, probs, acts, hid, pair, eout, rout = pl.pallas_call(
        functools.partial(exchange_kernel, nseq, ngrp),
        out_shape=(
            weights, weights, weights,
            jax.ShapeDtypeStruct((tokens, dim), BF16),
            jax.ShapeDtypeStruct((total_experts, tokens), F32),
            jax.ShapeDtypeStruct((2, rows, width), F32),
            jax.ShapeDtypeStruct((rows, width), BF16),
            jax.ShapeDtypeStruct((2, rows, dim), BF16),
            jax.ShapeDtypeStruct((total_experts, dim), BF16),
            jax.ShapeDtypeStruct((total_experts, dim), BF16),
        ),
        in_specs=[hspec] * 8,
        out_specs=(vspec,) * 10,
        scratch_shapes=[
            pltpu.VMEM((nseq, experts, dim), BF16),
            pltpu.VMEM((nseq, experts, dim), BF16),
            pltpu.VMEM((nseq, 2, experts, dim), BF16),
            pltpu.VMEM((ngrp, experts, dim), BF16),
            pltpu.VMEM((ngrp, experts, dim), BF16),
            DMA((5,)), DMA((3, experts)),
            DMA((nseq,)), DMA((nseq,)), DMA((nseq,)), DMA((nseq,)),
            DMA((ngrp,)), DMA((ngrp,)), DMA((ngrp,)), DMA((ngrp,)),
        ],
        compiler_params=pltpu.CompilerParams(
            collective_id=0, has_side_effects=True, vmem_limit_bytes=8 * 1024 * 1024),
        name="exchange",
    )(*(pltpu.with_memory_space_constraint(a, pltpu.HBM) for a in (
        out_grad, jnp.transpose(combine_logits[0]), expert_out, slot_in, router, w_gate, w_up, w_down)))

    cut = 256 if width % 256 == 0 else width
    gate_grad, mine, sends, grad_up, grad_down = pl.pallas_call(
        functools.partial(first_kernel, experts, cut),
        out_shape=(
            jax.ShapeDtypeStruct((rows, width), BF16),
            jax.ShapeDtypeStruct((experts, dim), F32),
            jax.ShapeDtypeStruct((max(ngrp - 1, 1), experts, dim), BF16),
            weights, weights,
        ),
        in_specs=[vspec] * 6,
        out_specs=(vspec,) * 3 + (hspec,) * 2,
        scratch_shapes=[
            pltpu.VMEM((2, experts, width, dim), BF16),
            DMA((2, experts, width // cut)),
        ],
        compiler_params=pltpu.CompilerParams(vmem_limit_bytes=26 * 1024 * 1024),
        name="first",
    )(gate_w, up_w, down_w, acts, hid, pair)

    got = [
        lax.ppermute(sends[d - 1], "grp", [(g, (g + d) % ngrp) for g in range(ngrp)])
        for d in range(1, ngrp)
    ]

    token_grad, grad_gate = pl.pallas_call(
        functools.partial(second_kernel, experts, cut),
        out_shape=(jax.ShapeDtypeStruct((1, tokens, dim), BF16), weights),
        in_specs=[vspec] * 6,
        out_specs=(hspec,) * 2,
        scratch_shapes=[
            pltpu.VMEM((experts, width, dim), BF16),
            pltpu.VMEM((tokens, dim), BF16),
            DMA((experts, width // cut)),
            DMA((1,)),
        ],
        compiler_params=pltpu.CompilerParams(vmem_limit_bytes=20 * 1024 * 1024),
        cost_estimate=pl.CostEstimate(
            flops=0, bytes_accessed=experts * width * dim * 2, transcendentals=0),
        name="second",
    )(gate_grad, pair, probs, grad, eout, rout)
    slot_grad = mine
    for part in got:
        slot_grad = slot_grad + part.astype(F32)
    return token_grad, slot_grad[None], grad_gate, grad_up, grad_down


def solution(mesh):
    return jax.shard_map(
        functools.partial(per_device, mesh.shape["seq"], mesh.shape["grp"]),
        mesh=mesh,
        in_specs=(
            P("grp", "seq", None),
            P("grp", "seq", None),
            P("grp", "seq", None),
            P("grp", "seq", None),
            P("seq", None),
            P("seq", "grp", None),
            P("seq", "grp", None),
            P("seq", "grp", None),
        ),
        out_specs=(
            P("grp", "seq", None),
            P("grp", "seq", None),
            P("seq", "grp", None),
            P("seq", "grp", None),
            P("seq", "grp", None),
        ),
        check_vma=False,
    )
```

```python
import functools

import jax
import jax.numpy as jnp
from jax import lax
from jax.experimental import pallas as pl
from jax.experimental.pallas import tpu as pltpu
from jax.sharding import PartitionSpec as P

MESH = pl.DeviceIdType.MESH
F32 = jnp.float32
BF16 = jnp.bfloat16
NT = (((1,), (1,)), ((), ()))
TN = (((0,), (0,)), ((), ()))


def rows_of(ref, count):
    return jnp.concatenate([ref[i].astype(F32) for i in range(count)], axis=0).astype(BF16)


def exchange_kernel(
    nseq, ngrp,
    grad_hbm, logit_hbm, eout_hbm, slot_hbm, router_hbm, gate_hbm, up_hbm, down_hbm,
    gate_w, up_w, down_w, grad, probs_ref, acts_ref, hid_ref, pair_ref, eout_ref, rout_ref,
    part_out, part_in, pieces, slots, outs,
    load_sem, w_sem, part_ssem, part_rsem, piece_ssem, piece_rsem,
    slot_ssem, slot_rsem, out_ssem, out_rsem,
):
    s_me = lax.axis_index("seq")
    g_me = lax.axis_index("grp")
    experts = slots.shape[1]

    barrier = pltpu.get_barrier_semaphore()

    def greet_seq(d, c):
        pl.semaphore_signal(barrier, inc=1, device_id={"seq": lax.rem(s_me + d, nseq)}, device_id_type=MESH)
        return c

    def greet_grp(d, c):
        pl.semaphore_signal(barrier, inc=1, device_id={"grp": lax.rem(g_me + d, ngrp)}, device_id_type=MESH)
        return c

    loads = [
        pltpu.make_async_copy(logit_hbm, probs_ref, load_sem.at[0]),
        pltpu.make_async_copy(grad_hbm.at[0], grad, load_sem.at[1]),
        pltpu.make_async_copy(slot_hbm.at[0], slots.at[g_me], load_sem.at[2]),
        pltpu.make_async_copy(eout_hbm.at[0], pieces.at[s_me, 0], load_sem.at[3]),
        pltpu.make_async_copy(router_hbm, pieces.at[s_me, 1], load_sem.at[4]),
    ]
    for c in loads:
        c.start()

    lax.fori_loop(1, ngrp, greet_grp, 0)
    lax.fori_loop(1, nseq, greet_seq, 0)
    w_loads = {}
    for m, (src, dst) in enumerate(((gate_hbm, gate_w), (up_hbm, up_w), (down_hbm, down_w))):
        for e in range(experts):
            w_loads[m, e] = pltpu.make_async_copy(src.at[e], dst.at[e], w_sem.at[m, e])

    def part_copy(d):
        to = lax.rem(s_me + d, nseq)
        return pltpu.make_async_remote_copy(
            src_ref=part_out.at[to], dst_ref=part_in.at[s_me],
            send_sem=part_ssem.at[to], recv_sem=part_rsem.at[s_me],
            device_id={"seq": to}, device_id_type=MESH)

    def piece_copy(d):
        to = lax.rem(s_me + d, nseq)
        return pltpu.make_async_remote_copy(
            src_ref=pieces.at[s_me], dst_ref=pieces.at[s_me],
            send_sem=piece_ssem.at[to], recv_sem=piece_rsem.at[s_me],
            device_id={"seq": to}, device_id_type=MESH)

    def grp_copy(d, buf, ssem, rsem):
        to = lax.rem(g_me + d, ngrp)
        return pltpu.make_async_remote_copy(
            src_ref=buf.at[g_me], dst_ref=buf.at[g_me],
            send_sem=ssem.at[to], recv_sem=rsem.at[g_me],
            device_id={"grp": to}, device_id_type=MESH)

    def seq_arrived(d, buf, rsem, ssem):
        at = lax.rem(s_me + d, nseq)
        pltpu.make_async_remote_copy(
            src_ref=buf.at[at], dst_ref=buf.at[at], send_sem=ssem.at[at], recv_sem=rsem.at[at],
            device_id={"seq": at}, device_id_type=MESH).wait_recv()

    def grp_arrived(d, buf, rsem, ssem):
        at = lax.rem(g_me + d, ngrp)
        pltpu.make_async_remote_copy(
            src_ref=buf.at[at], dst_ref=buf.at[at], send_sem=ssem.at[at], recv_sem=rsem.at[at],
            device_id={"grp": at}, device_id_type=MESH).wait_recv()

    def each(low, high, fn):
        def step(d, c):
            fn(d)
            return c
        lax.fori_loop(low, high, step, 0)

    loads[0].wait()
    z = probs_ref[...]
    z = jnp.exp(z - jnp.max(z, axis=0, keepdims=True))
    probs = z / jnp.sum(z, axis=0, keepdims=True)
    probs_ref[...] = probs
    loads[1].wait()
    for e in range(experts):
        w_loads[0, e].start()
        w_loads[1, e].start()
    for e in range(experts):
        w_loads[2, e].start()
    share = jnp.dot(probs.astype(BF16), grad[...], preferred_element_type=F32)
    for j in range(nseq):
        part_out[j] = share[j * experts:(j + 1) * experts].astype(BF16)
    part_in[s_me] = part_out[s_me]
    for c in loads[2:]:
        c.wait()

    pl.semaphore_wait(barrier, (nseq - 1) + (ngrp - 1))
    each(1, nseq, lambda d: part_copy(d).start())
    each(1, ngrp, lambda d: grp_copy(d, slots, slot_ssem, slot_rsem).start())
    each(1, nseq, lambda d: piece_copy(d).start())

    rows = ngrp * experts
    width = gate_w.shape[1]
    own = lax.rem(lax.broadcasted_iota(jnp.int32, (rows, width), 0), experts)

    each(1, ngrp, lambda d: grp_arrived(d, slots, slot_rsem, slot_ssem))
    x = rows_of(slots, ngrp)
    pair_ref[0] = x

    gate = jnp.zeros((rows, width), F32)
    upper = jnp.zeros((rows, width), F32)

    def project(e, gate, upper):
        w_loads[0, e].wait()
        gate = jnp.where(own == e, lax.dot_general(x, gate_w[e], NT, preferred_element_type=F32), gate)
        w_loads[1, e].wait()
        upper = jnp.where(own == e, lax.dot_general(x, up_w[e], NT, preferred_element_type=F32), upper)
        return gate, upper

    early = experts // 2
    for e in range(early):
        gate, upper = project(e, gate, upper)

    each(1, nseq, lambda d: seq_arrived(d, part_in, part_rsem, part_ssem))
    outs[g_me] = jnp.sum(part_in[...].astype(F32), axis=0).astype(BF16)
    each(1, ngrp, lambda d: grp_copy(d, outs, out_ssem, out_rsem).start())

    for e in range(early, experts):
        gate, upper = project(e, gate, upper)
    sig = jax.nn.sigmoid(gate)
    act = gate * sig
    hid_ref[...] = (act * upper).astype(BF16)
    acts_ref[0] = upper * sig * (1.0 + gate * (1.0 - sig))
    acts_ref[1] = act

    for e in range(experts):
        w_loads[2, e].wait()
    each(1, ngrp, lambda d: grp_arrived(d, outs, out_rsem, out_ssem))
    pair_ref[1] = rows_of(outs, ngrp)

    each(1, nseq, lambda d: seq_arrived(d, pieces, piece_rsem, piece_ssem))
    eout_ref[...] = rows_of(pieces.at[:, 0], nseq)
    rout_ref[...] = rows_of(pieces.at[:, 1], nseq)

    each(1, nseq, lambda d: part_copy(d).wait_send())
    each(1, nseq, lambda d: piece_copy(d).wait_send())
    each(1, ngrp, lambda d: grp_copy(d, slots, slot_ssem, slot_rsem).wait_send())
    each(1, ngrp, lambda d: grp_copy(d, outs, out_ssem, out_rsem).wait_send())


def mxu_outer(a, v, dst):
    dst[...] = lax.dot_general(a, v, TN, preferred_element_type=F32).astype(BF16)


def picker(experts, e, rows, lanes=128):
    row = lax.broadcasted_iota(jnp.int32, (rows, lanes * (rows // experts)), 0)
    lane = lax.broadcasted_iota(jnp.int32, (rows, lanes * (rows // experts)), 1)
    return jnp.where(row == (lane // lanes) * experts + e, 1.0, 0.0).astype(BF16)


def vpu_outer(experts, e, a, v, dst, lanes=128, step=16):
    rows, dim = v.shape
    spread = lax.dot_general(a, picker(experts, e, rows, lanes), TN, preferred_element_type=F32).astype(BF16)
    tiles = [
        [jnp.broadcast_to(v[r:r + 1, l:l + lanes], (step, lanes)) for l in range(0, dim, lanes)]
        for r in range(e, rows, experts)
    ]
    for i in range(0, a.shape[1], step):
        out = []
        for l in range(dim // lanes):
            total = None
            for g, row in enumerate(tiles):
                term = spread[i:i + step, g * lanes:(g + 1) * lanes] * row[l]
                total = term if total is None else total + term
            out.append(total)
        dst[i:i + step] = jnp.concatenate(out, axis=1)


def first_kernel(
    experts, cut,
    gate_w, up_w, down_w, acts_ref, hid_ref, pair_ref,
    gg_ref, mine_ref, send_ref, gu_hbm, gd_hbm,
    staged, sem,
):
    outs = (gd_hbm, gu_hbm)
    rows, width = hid_ref.shape
    ngrp = rows // experts
    own = lax.rem(lax.broadcasted_iota(jnp.int32, (rows, cut), 0), experts)
    x, so = pair_ref[0], pair_ref[1]

    def chunk(k, e, j):
        at = pl.ds(j * cut, cut)
        return pltpu.make_async_copy(staged.at[k, e, at], outs[k].at[e, at], sem.at[k, e, j])

    def put(k, e, j, a, v):
        vpu_outer(experts, e, a, v, staged.at[k, e, pl.ds(j * cut, cut)])
        chunk(k, e, j).start()

    def spread(e, j, gate_grad, up_grad, total):
        at = slice(j * cut, (j + 1) * cut)
        total += jnp.dot(gate_grad, gate_w[e, at], preferred_element_type=F32)
        total += jnp.dot(up_grad, up_w[e, at], preferred_element_type=F32)
        put(1, e, j, up_grad, x)
        return total

    total = jnp.zeros((rows, x.shape[1]), F32)
    gate_all = [jnp.zeros((rows, cut), F32)] * (width // cut)
    late = []
    spots = [(e, j) for e in range(experts) for j in range(width // cut)]
    lead = 1

    def down(t):
        e, j = spots[t]
        put(0, e, j, hid_ref[:, j * cut:(j + 1) * cut], so)

    for t in range(lead):
        down(t)
    for t, (e, j) in enumerate(spots):
        at = slice(j * cut, (j + 1) * cut)
        hgrad = lax.dot_general(so, down_w[e, at], NT, preferred_element_type=F32)
        if t + lead < len(spots):
            down(t + lead)
        gate_f = jnp.where(own == e, hgrad * acts_ref[0, :, at], 0.0)
        gate_all[j] += gate_f
        up_grad = jnp.where(own == e, hgrad * acts_ref[1, :, at], 0.0).astype(BF16)
        late.append((e, j, gate_f.astype(BF16), up_grad))
        if len(late) > 1:
            total = spread(*late.pop(0), total)
    for item in late:
        total = spread(*item, total)
    for j in range(width // cut):
        gg_ref[:, j * cut:(j + 1) * cut] = gate_all[j].astype(BF16)
    g_me = lax.axis_index("grp")
    for d in range(ngrp):
        at = lax.rem(g_me + d, ngrp)
        piece = jnp.zeros((experts, total.shape[1]), F32)
        for g in range(ngrp):
            piece = jnp.where(at == g, total[g * experts:(g + 1) * experts], piece)
        if d == 0:
            mine_ref[...] = piece
        else:
            send_ref[d - 1] = piece.astype(BF16)
    for k in range(2):
        for e in range(experts):
            for j in range(width // cut):
                chunk(k, e, j).wait()


def second_kernel(
    experts, cut,
    gg_ref, pair_ref, probs_ref, grad_ref, eout_ref, rout_ref,
    tgrad_hbm, gg_hbm,
    staged, tokens, sem, small_sem,
):
    rows, width = gg_ref.shape

    def chunk(e, j):
        at = pl.ds(j * cut, cut)
        return pltpu.make_async_copy(staged.at[e, at], gg_hbm.at[e, at], sem.at[e, j])

    x = pair_ref[0]
    for e in range(experts):
        for j in range(width // cut):
            at = slice(j * cut, (j + 1) * cut)
            vpu_outer(experts, e, gg_ref[:, at], x, staged.at[e, at])
            chunk(e, j).start()
            if e * (width // cut) + j == min(11, experts * (width // cut) - 1):
                wgrad = lax.dot_general(eout_ref[...], grad_ref[...], NT, preferred_element_type=F32)
                p = probs_ref[...]
                centre = jnp.sum(wgrad * p, axis=0, keepdims=True)
                lgrad = (p * (wgrad - centre)).astype(BF16)
                tokens[...] = lax.dot_general(lgrad, rout_ref[...], TN, preferred_element_type=F32).astype(BF16)
                small = pltpu.make_async_copy(tokens, tgrad_hbm.at[0], small_sem.at[0])
                small.start()
    for e in range(experts):
        for j in range(width // cut):
            chunk(e, j).wait()
    small.wait()


def per_device(nseq, ngrp, out_grad, combine_logits, expert_out, slot_in, router, w_gate, w_up, w_down):
    _, tokens, dim = out_grad.shape
    total_experts = combine_logits.shape[2]
    experts, width, _ = w_gate.shape
    rows = ngrp * experts
    DMA = pltpu.SemaphoreType.DMA
    hspec = pl.BlockSpec(memory_space=pltpu.HBM)
    vspec = pl.BlockSpec(memory_space=pltpu.VMEM)
    weights = jax.ShapeDtypeStruct((experts, width, dim), BF16)
    gate_w, up_w, down_w, grad, probs, acts, hid, pair, eout, rout = pl.pallas_call(
        functools.partial(exchange_kernel, nseq, ngrp),
        out_shape=(
            weights, weights, weights,
            jax.ShapeDtypeStruct((tokens, dim), BF16),
            jax.ShapeDtypeStruct((total_experts, tokens), F32),
            jax.ShapeDtypeStruct((2, rows, width), F32),
            jax.ShapeDtypeStruct((rows, width), BF16),
            jax.ShapeDtypeStruct((2, rows, dim), BF16),
            jax.ShapeDtypeStruct((total_experts, dim), BF16),
            jax.ShapeDtypeStruct((total_experts, dim), BF16),
        ),
        in_specs=[hspec] * 8,
        out_specs=(vspec,) * 10,
        scratch_shapes=[
            pltpu.VMEM((nseq, experts, dim), BF16),
            pltpu.VMEM((nseq, experts, dim), BF16),
            pltpu.VMEM((nseq, 2, experts, dim), BF16),
            pltpu.VMEM((ngrp, experts, dim), BF16),
            pltpu.VMEM((ngrp, experts, dim), BF16),
            DMA((5,)), DMA((3, experts)),
            DMA((nseq,)), DMA((nseq,)), DMA((nseq,)), DMA((nseq,)),
            DMA((ngrp,)), DMA((ngrp,)), DMA((ngrp,)), DMA((ngrp,)),
        ],
        compiler_params=pltpu.CompilerParams(
            collective_id=0, has_side_effects=True, vmem_limit_bytes=8 * 1024 * 1024),
        name="exchange",
    )(*(pltpu.with_memory_space_constraint(a, pltpu.HBM) for a in (
        out_grad, jnp.transpose(combine_logits[0]), expert_out, slot_in, router, w_gate, w_up, w_down)))

    cut = 256 if width % 256 == 0 else width
    gate_grad, mine, sends, grad_up, grad_down = pl.pallas_call(
        functools.partial(first_kernel, experts, cut),
        out_shape=(
            jax.ShapeDtypeStruct((rows, width), BF16),
            jax.ShapeDtypeStruct((experts, dim), F32),
            jax.ShapeDtypeStruct((max(ngrp - 1, 1), experts, dim), BF16),
            weights, weights,
        ),
        in_specs=[vspec] * 6,
        out_specs=(vspec,) * 3 + (hspec,) * 2,
        scratch_shapes=[
            pltpu.VMEM((2, experts, width, dim), BF16),
            DMA((2, experts, width // cut)),
        ],
        compiler_params=pltpu.CompilerParams(vmem_limit_bytes=26 * 1024 * 1024),
        name="first",
    )(gate_w, up_w, down_w, acts, hid, pair)

    got = [
        lax.ppermute(sends[d - 1], "grp", [(g, (g + d) % ngrp) for g in range(ngrp)])
        for d in range(1, ngrp)
    ]

    token_grad, grad_gate = pl.pallas_call(
        functools.partial(second_kernel, experts, cut),
        out_shape=(jax.ShapeDtypeStruct((1, tokens, dim), BF16), weights),
        in_specs=[vspec] * 6,
        out_specs=(hspec,) * 2,
        scratch_shapes=[
            pltpu.VMEM((experts, width, dim), BF16),
            pltpu.VMEM((tokens, dim), BF16),
            DMA((experts, width // cut)),
            DMA((1,)),
        ],
        compiler_params=pltpu.CompilerParams(vmem_limit_bytes=20 * 1024 * 1024),
        cost_estimate=pl.CostEstimate(
            flops=0, bytes_accessed=experts * width * dim * 2, transcendentals=0),
        name="second",
    )(gate_grad, pair, probs, grad, eout, rout)
    slot_grad = mine
    for part in got:
        slot_grad = slot_grad + part.astype(F32)
    return token_grad, slot_grad[None], grad_gate, grad_up, grad_down


def solution(mesh):
    return jax.shard_map(
        functools.partial(per_device, mesh.shape["seq"], mesh.shape["grp"]),
        mesh=mesh,
        in_specs=(
            P("grp", "seq", None),
            P("grp", "seq", None),
            P("grp", "seq", None),
            P("grp", "seq", None),
            P("seq", None),
            P("seq", "grp", None),
            P("seq", "grp", None),
            P("seq", "grp", None),
        ),
        out_specs=(
            P("grp", "seq", None),
            P("grp", "seq", None),
            P("seq", "grp", None),
            P("seq", "grp", None),
            P("seq", "grp", None),
        ),
        check_vma=False,
    )
```
